32 devices in a mesh: gx: 2 (over y), gy: 4 (over x, core), gz: 4 (over z).
Axes of the slice: x: 2, y: 2, z: 4, core: 2. Of those that a mesh axis runs over, the one named last changes fastest.
Arguments:
- source: bfloat16 [512, 512, 512], P('gz', 'gx', 'gy'), may hold values from -6 to 6
- forward_x: bfloat16 [512, 512], replicated, may hold values from -0.25 to 0.25
- forward_y: bfloat16 [512, 512], replicated, may hold values from -0.25 to 0.25
- forward_z: bfloat16 [512, 512], replicated, may hold values from -0.25 to 0.25
- inverse_x: bfloat16 [512, 512], replicated, may hold values from -0.25 to 0.25
- inverse_y: bfloat16 [512, 512], replicated, may hold values from -0.25 to 0.25
- inverse_z: bfloat16 [512, 512], replicated, may hold values from -0.25 to 0.25
- values_x: float32 [512], replicated, may hold values from 0.1 to 2
- values_y: float32 [512], replicated, may hold values from 0.1 to 2
- values_z: float32 [512], replicated, may hold values from 0.1 to 2
Outputs:
- solution: bfloat16 [512, 512, 512], P('gz', 'gx', 'gy')
The draws below stay inside these ranges and needn't reach their ends.
All inputs are finite; a program needn't handle non-finite values.
Results may differ from the reference program's by a relative error of at most 0.015.
Values may be sent and summed in bfloat16 or wider, within the bound.
No kernel may reach another device: no remote copies, remote signals or barrier semaphores. Data moves between devices by JAX's collectives and lax.ppermute only.
A program may use at most 128 MiB of HBM per device.

```python
import math
import jax
import jax.numpy as jnp
from jax import lax

NX = 512
NY = 512
NZ = 512


def block_levels(rng, shape, cuts, least, high):
    def one(dim, blocks):
        steps = jax.random.uniform(jax.random.fold_in(jax.random.fold_in(rng, 6), dim), (blocks,), jnp.float32, least / len(cuts), high / len(cuts))
        return jnp.repeat(jnp.exp(steps), shape[dim] // blocks).reshape((-1,) + (1,) * (len(shape) - dim - 1))

    loudness = one(*cuts[0])
    for cut in cuts[1:]:
        loudness = loudness * one(*cut)
    return loudness


def scatter_about(own_key, dims, deviation, most, pieces=(), kind=jnp.bfloat16):
    loudness = block_levels(own_key, dims, pieces, -0.22, 0.18) if pieces else 1.0
    drawn = jax.random.normal(own_key, dims, jnp.float32) * deviation * loudness
    return jnp.minimum(jnp.maximum(drawn, -most), most).astype(kind)


def setup_inputs(seed: int = 0) -> dict:
    streams_of = jax.random.split(jax.random.key(seed), 11)
    source = scatter_about(streams_of[0], (NZ, NY, NX), 1.0, 6.0, ((0, 4), (1, 2), (2, 4)))
    forward_x = scatter_about(streams_of[1], (NX, NX), NX ** -0.5, 0.25)
    forward_y = scatter_about(streams_of[2], (NY, NY), NY ** -0.5, 0.25)
    forward_z = scatter_about(streams_of[3], (NZ, NZ), NZ ** -0.5, 0.25)
    inverse_x = scatter_about(streams_of[4], (NX, NX), NX ** -0.5, 0.25)
    inverse_y = scatter_about(streams_of[5], (NY, NY), NY ** -0.5, 0.25)
    inverse_z = scatter_about(streams_of[6], (NZ, NZ), NZ ** -0.5, 0.25)
    values_x = jnp.clip(jnp.exp(jax.random.uniform(streams_of[7], (NX,), jnp.float32, math.log(0.1), math.log(2.0))), 0.1, 2.0)
    values_y = jnp.clip(jnp.exp(jax.random.uniform(streams_of[8], (NY,), jnp.float32, math.log(0.1), math.log(2.0))), 0.1, 2.0)
    values_z = jnp.clip(jnp.exp(jax.random.uniform(streams_of[9], (NZ,), jnp.float32, math.log(0.1), math.log(2.0))), 0.1, 2.0)
    return {"source": source, "forward_x": forward_x, "forward_y": forward_y, "forward_z": forward_z, "inverse_x": inverse_x, "inverse_y": inverse_y, "inverse_z": inverse_z, "values_x": values_x, "values_y": values_y, "values_z": values_z}


def along_x(data, basis):
    depth, rows, cols = data.shape
    flat = data.reshape(depth * rows, cols)
    out = jnp.dot(flat, basis.T, preferred_element_type=jnp.float32)
    return out.astype(jnp.bfloat16).reshape(depth, rows, basis.shape[0])


def along_y(data, basis):
    def single(plane):
        return jnp.dot(basis, plane, preferred_element_type=jnp.float32).astype(jnp.bfloat16)
    return lax.map(single, data)


def along_z(data, basis):
    depth, rows, cols = data.shape
    out = jnp.dot(basis, data.reshape(depth, rows * cols), preferred_element_type=jnp.float32)
    return out.astype(jnp.bfloat16).reshape(basis.shape[0], rows, cols)


def reference(source, forward_x, forward_y, forward_z, inverse_x, inverse_y, inverse_z, values_x, values_y, values_z):
    step_a = along_x(source, forward_x)
    step_b = along_y(step_a, forward_y)
    step_c = along_z(step_b, forward_z)
    denom = values_z[:, None, None] + values_y[None, :, None] + values_x[None, None, :]
    scaled = (step_c.astype(jnp.float32) / denom).astype(jnp.bfloat16)
    step_d = along_z(scaled, inverse_z)
    step_e = along_y(step_d, inverse_y)
    return along_x(step_e, inverse_x)
```

```python
import functools

import jax
import jax.numpy as jnp
from jax import lax
from jax.experimental import pallas as pl
from jax.experimental.pallas import tpu as pltpu
from jax.sharding import PartitionSpec as P


FORWARD_SIZES = (1,)*8
BACKWARD_SIZES = (1,)*8
AHEAD = {'S':2,'W':2}
SENDS = {"S": "gx", "G": "gy", "Z": "gz", "W": "gz", "H": "gy", "T": "gx"}
ROWS = 8
F32 = jnp.float32
BF16 = jnp.bfloat16


def dot(a, b):
    return jnp.dot(a, b, preferred_element_type=F32)


def params(**kw):
    return pltpu.CompilerParams(vmem_limit_bytes=48 * 1024 * 1024, **kw)


def cost(flops, nbytes):
    return pl.CostEstimate(flops=flops, bytes_accessed=nbytes, transcendentals=0)


ANY = pl.BlockSpec(memory_space=pl.ANY)


def chunks(depth, sizes):
    rows = [n * depth // sum(sizes) for n in sizes]
    by_z = [0, len(rows) - 1] + list(range(1, len(rows) - 1))
    starts = [0] * len(rows)
    for a, b in zip(by_z, by_z[1:]):
        starts[b] = starts[a] + rows[a]
    return rows, starts, by_z


def forward_order():
    n = len(FORWARD_SIZES)
    ahead = AHEAD["S"]
    steps = [f"{kind}{c}" for c in range(ahead) for kind in "CS"]
    for c in range(n):
        steps += [f"F{c}", f"G{c}"]
        steps += [f"{kind}{c + ahead}" for kind in "CS" if c + ahead < n]
        steps += [f"A{c}", f"Z{c}"]
    return steps


def backward_order():
    n = len(BACKWARD_SIZES)
    steps = [f"W{c}" for c in range(AHEAD["W"])]
    for c in range(n):
        steps += [f"B{c}", f"H{c}"] + [f"W{c + AHEAD['W']}"] * (c + AHEAD["W"] < n)
        steps += [f"P{c}", f"T{c}"] + [f"R{c - 2}"] * (c > 1)
    return steps + [f"R{n - 2}", f"R{n - 1}"]


def partners(count):
    return list(range(2, count)) + [1]


def places(index, count):
    return [index ^ k for k in range(count)]


def cut(ref, height, row, width, col):
    return ref[
        pl.ds(pl.multiple_of(row * height, height), height),
        pl.ds(pl.multiple_of(col * width, width), width),
    ]


def forward_y_kernel(*refs, count, outs):
    place, pieces, basis, out = refs[0], refs[1 : 1 + count], refs[1 + count], refs[-outs:]
    steps, rows, cols = pieces[0].shape
    width = basis.shape[0] // count // outs
    own = jnp.concatenate(
        [
            jnp.concatenate([cut(basis, width, r, rows, c) for c in places(place[0], count)], axis=1)
            for r in places(place[0] * outs + place[1], outs)
        ],
        axis=0,
    )

    def pair(i, carry):
        z = 2 * i
        rhs = jnp.concatenate(
            [jnp.concatenate([ref[z], ref[z + 1]], axis=1) for ref in pieces], axis=0
        )
        acc = dot(own, rhs).astype(BF16)
        for k in range(outs):
            block = acc[k * width : (k + 1) * width]
            out[k][z] = block[:, :cols]
            out[k][z + 1] = block[:, cols:]
        return carry

    lax.fori_loop(0, steps // 2, pair, 0, unroll=4)


def forward_y(place, own, start, others, basis, outs, after=()):
    zc, rows, cols = others[0].shape
    count = 1 + len(others)
    q = basis.shape[0] // count
    first = start // ROWS
    spec = pl.BlockSpec((ROWS, rows, cols), lambda i, s: (i, 0, 0))
    return pl.pallas_call(
        functools.partial(forward_y_kernel, count=count, outs=outs),
        grid_spec=pltpu.PrefetchScalarGridSpec(
            num_scalar_prefetch=1,
            grid=(zc // ROWS,),
            in_specs=[pl.BlockSpec((ROWS, rows, cols), lambda i, s: (i + first, 0, 0))]
            + [spec] * len(others)
            + [pl.BlockSpec(basis.shape, lambda i, s: (0, 0))]
            + [ANY] * len(after),
            out_specs=[pl.BlockSpec((ROWS, q // outs, cols), lambda i, s: (i, 0, 0))] * outs,
        ),
        out_shape=[jax.ShapeDtypeStruct((zc, q // outs, cols), BF16)] * outs,
        compiler_params=params(),
        cost_estimate=cost(2 * zc * q * basis.shape[1] * cols, 2 * zc * cols * (basis.shape[1] + q)),
        name="forward_y",
    )(place, own, *others, basis, *after)


def along_x_kernel(*refs, count, outs, axes):
    place, pieces, basis = refs[0], refs[1 : 1 + count], refs[1 + count]
    out, scratch = refs[-1 - outs : -1], refs[-1]
    a, b, cols = pieces[0].shape
    pitch = scratch.shape[1] // a
    width = basis.shape[0] // outs
    lhs = jnp.concatenate([ref[...].reshape(a * b, cols) for ref in pieces], axis=1)
    for k, row in enumerate(places(place[axes[1]], outs)):
        rhs = jnp.concatenate(
            [cut(basis, width, row, cols, c) for c in places(place[axes[0]], count)], axis=1
        )
        acc = lax.dot_general(lhs, rhs, (((1,), (1,)), ((), ())), preferred_element_type=F32)
        for i in range(a):
            scratch[k % 2, i * pitch : i * pitch + b, :] = acc[i * b : (i + 1) * b]
        for j in range(b):
            out[k][j] = scratch[k % 2, pl.ds(j, a, stride=pitch), :].astype(BF16)


def along_x(place, pieces, basis, outs, rows_first, after=()):
    cols = pieces[0].shape[2]
    width = basis.shape[0] // outs
    zc, q = pieces[0].shape[:2] if rows_first else pieces[0].shape[1::-1]
    z_major = ((ROWS, q), lambda i, s: (i, 0, 0))
    q_major = ((q, ROWS), lambda i, s: (0, i, 0))
    src, dst = (z_major, q_major) if rows_first else (q_major, z_major)
    shape = (q, zc, width) if rows_first else (zc, q, width)
    pitch = src[0][1] + 8
    return pl.pallas_call(
        functools.partial(
            along_x_kernel, count=len(pieces), outs=outs, axes=(1, 2) if rows_first else (2, 1)
        ),
        grid_spec=pltpu.PrefetchScalarGridSpec(
            num_scalar_prefetch=1,
            grid=(zc // ROWS,),
            in_specs=[pl.BlockSpec(src[0] + (cols,), src[1])] * len(pieces)
            + [pl.BlockSpec(basis.shape, lambda i, s: (0, 0))]
            + [ANY] * len(after),
            out_specs=[pl.BlockSpec(dst[0] + (width,), dst[1])] * outs,
            scratch_shapes=[pltpu.VMEM((2, src[0][0] * pitch, width), F32)],
        ),
        out_shape=[jax.ShapeDtypeStruct(shape, BF16)] * outs,
        compiler_params=params(),
        cost_estimate=cost(2 * zc * q * basis.shape[0] * basis.shape[1], 2 * zc * q * sum(basis.shape)),
        name="along_x",
    )(place, *pieces, basis, *after)


def lines_kernel(*refs, count, outs, step):
    place, lam_y, pieces = refs[0], refs[1], refs[2 : 2 + count]
    forward, inverse, base = refs[2 + count : 5 + count]
    out, there, back_again = refs[-2 - outs : -2], refs[-2], refs[-1]
    first = pl.program_id(0) * step
    depth, cols = base.shape

    @pl.when(pl.program_id(0) == 0)
    def _():
        n = there.shape[0]
        size = depth // n
        for k, block in enumerate(places(place[2], n)):
            there[k] = forward[:, pl.ds(pl.multiple_of(block * size, size), size)]
            back_again[k * size : (k + 1) * size] = inverse[pl.ds(pl.multiple_of(block * size, size), size), :]

    lhs = jnp.concatenate([there[k] for k in range(there.shape[0])], axis=1)
    for q in range(0, step, 2):
        rhs = jnp.concatenate(
            [jnp.concatenate([ref[q], ref[q + 1]], axis=1) for ref in pieces], axis=0
        )
        acc = dot(lhs, rhs).astype(BF16).astype(F32)
        left = acc[:, :cols] / (base[...] + lam_y[first + q])
        right = acc[:, cols:] / (base[...] + lam_y[first + q + 1])
        back = dot(back_again[...], jnp.concatenate([left, right], axis=1).astype(BF16)).astype(BF16)
        row = 0
        for ref in out:
            stop = row + ref.shape[1]
            ref[q] = back[row:stop, :cols]
            ref[q + 1] = back[row:stop, cols:]
            row = stop


def lines(place, pieces, forward, inverse, base, lam_y, parts, sizes):
    q, _, cols = pieces[0].shape
    depth = forward.shape[0]
    step = 8
    spec = lambda n: pl.BlockSpec((step, n, cols), lambda i, s, t: (i, 0, 0))
    whole = lambda x: pl.BlockSpec(x.shape, lambda i, s, t: (0, 0))
    outs = [n for _ in range(parts) for n in sizes]
    return pl.pallas_call(
        functools.partial(lines_kernel, count=len(pieces), outs=len(outs), step=step),
        grid_spec=pltpu.PrefetchScalarGridSpec(
            num_scalar_prefetch=2,
            grid=(q // step,),
            in_specs=[spec(p.shape[1]) for p in pieces] + [whole(forward), whole(inverse), whole(base)],
            out_specs=[spec(n) for n in outs],
            scratch_shapes=[
                pltpu.VMEM((parts, depth, depth // parts), BF16),
                pltpu.VMEM((depth, depth), BF16),
            ],
        ),
        out_shape=[jax.ShapeDtypeStruct((q, n, cols), BF16) for n in outs],
        compiler_params=params(),
        cost_estimate=cost(4 * q * cols * depth * depth, 4 * q * cols * depth),
        name="lines",
    )(place, lam_y, *pieces, forward, inverse, base)


def inverse_y_kernel(*refs, count, adds, to):
    place, pieces, basis = refs[0], refs[1 : 1 + count], refs[1 + count]
    partials, out, there = refs[2 + count : 2 + count + adds], refs[-2], refs[-1]
    _, q, cols = pieces[0].shape
    rows = out.shape[1]
    own = cut(basis, rows, place[0] ^ to, count * q, place[0])
    for ref, k in zip(pieces, places(place[1], count)):
        there[k] = ref[...]

    def pair(i, carry):
        z = 2 * i
        rhs = jnp.concatenate(
            [jnp.concatenate([there[k, z], there[k, z + 1]], axis=1) for k in range(count)], axis=0
        )
        acc = dot(own, rhs)
        left, right = acc[:, :cols], acc[:, cols:]
        for ref in partials:
            left = left + ref[z].astype(F32)
            right = right + ref[z + 1].astype(F32)
        out[z] = left.astype(BF16)
        out[z + 1] = right.astype(BF16)
        return carry

    lax.fori_loop(0, out.shape[0] // 2, pair, 0, unroll=4)


def inverse_y(place, pieces, basis, to, rows, after=(), partials=(), into=None, start=0, depth=None):
    zc, q, cols = pieces[0].shape
    first = start // ROWS
    part = pl.BlockSpec((ROWS, rows, cols), lambda i, s: (i, 0, 0))
    extra = [] if into is None else [into]
    count = len(pieces)
    return pl.pallas_call(
        functools.partial(inverse_y_kernel, count=count, adds=len(partials), to=to),
        grid_spec=pltpu.PrefetchScalarGridSpec(
            num_scalar_prefetch=1,
            grid=(zc // ROWS,),
            in_specs=[pl.BlockSpec((ROWS, q, cols), lambda i, s: (i, 0, 0))] * count
            + [pl.BlockSpec(basis.shape, lambda i, s: (0, 0))]
            + [part] * len(partials)
            + [ANY] * (len(extra) + len(after)),
            out_specs=pl.BlockSpec((ROWS, rows, cols), lambda i, s: (i + first, 0, 0)),
            scratch_shapes=[pltpu.VMEM((count, ROWS, q, cols), BF16)],
        ),
        out_shape=jax.ShapeDtypeStruct((depth or zc, rows, cols), BF16),
        input_output_aliases={count + 2 + len(partials): 0} if extra else {},
        compiler_params=params(),
        cost_estimate=cost(2 * zc * rows * count * q * cols, 2 * zc * cols * (count * q + rows)),
        name="inverse_y",
    )(place, *pieces, basis, *partials, *extra, *after)


def swap(value, axis, k):
    count = lax.axis_size(axis)
    return lax.ppermute(value, axis, [(i, i ^ k) for i in range(count)])


def exchange(step, pieces):
    axis = SENDS[step[0]]
    out = list(pieces)
    for k in partners(len(pieces)):
        out[k] = swap(pieces[k], axis, k)
    return out


def copy_kernel(source, out):
    out[...] = source[...]


def copy_rows(source, start, count):
    first = start // ROWS
    block = (ROWS,) + source.shape[1:]
    return pl.pallas_call(
        copy_kernel,
        grid=(count // block[0],),
        in_specs=[pl.BlockSpec(block, lambda i: (i + first, 0, 0))],
        out_specs=pl.BlockSpec(block, lambda i: (i, 0, 0)),
        out_shape=jax.ShapeDtypeStruct((count,) + source.shape[1:], BF16),
        compiler_params=params(),
        name="copy_rows",
    )(source)


def on_device(
    source, forward_x, forward_y_basis, forward_z, inverse_x, inverse_y_basis, inverse_z,
    values_x, values_y, values_z,
):
    ny, ng, nz = lax.axis_size("gx"), lax.axis_size("gy"), lax.axis_size("gz")
    iy, ig, iz = lax.axis_index("gx"), lax.axis_index("gy"), lax.axis_index("gz")
    place = jnp.stack([iy, ig, iz]).astype(jnp.int32)
    depth, rows, _ = source.shape
    slim = values_y.shape[0] // ny // ng
    width = values_x.shape[0] // nz
    lam_y = lax.dynamic_slice_in_dim(values_y, (iy * ng + ig) * slim, slim)
    lam_x = lax.dynamic_slice_in_dim(values_x, iz * width, width)
    base = values_z[:, None] + lam_x[None, :]

    sizes, starts, by_z = chunks(depth, FORWARD_SIZES)
    have = {}
    for step in forward_order():
        kind, c = step[0], int(step[1:])
        if kind in "CFA":
            if kind == "C":
                have[step] = copy_rows(source, starts[c], sizes[c])
            elif kind == "F":
                have[step] = forward_y(
                    place, source, starts[c], have[f"S{c}"], forward_y_basis, ng
                )
            else:
                have[step] = along_x(place, have[f"G{c}"], forward_x, nz, True)
        elif kind == "S":
            have[step] = exchange(step, [have[f"C{c}"]] * ny)[1:]
        else:
            have[step] = exchange(step, have[f"{'F' if kind == 'G' else 'A'}{c}"])

    flat = [have[f"Z{c}"][k] for k in range(nz) for c in by_z]
    sizes, starts, by_z = chunks(depth, BACKWARD_SIZES)
    count = len(sizes)
    flat = lines(place, flat, forward_z, inverse_z, base, lam_y, nz, [sizes[c] for c in by_z])

    result = None
    for step in backward_order():
        kind, c = step[0], int(step[1:])
        if kind == "W":
            have[step] = exchange(step, [flat[k * count + by_z.index(c)] for k in range(nz)])
        elif kind == "H":
            have[step] = exchange(step, have[f"B{c}"])
        elif kind == "T":
            have[step] = exchange(step, [None] + have[f"P{c}"])[1:]
        elif kind == "P":
            have[step] = [None] * (ny - 1)
            for k in partners(ny):
                have[step][k - 1] = inverse_y(place, have[f"H{c}"], inverse_y_basis, k, rows)
        else:
            if kind == "B":
                have[step] = along_x(place, have[f"W{c}"], inverse_x, ng, False)
            else:
                result = inverse_y(
                    place, have[f"H{c}"], inverse_y_basis, 0, rows, (),
                    have[f"T{c}"], result, starts[c], depth,
                )
    return result


def plain(data, basis, spec):
    return jnp.einsum(spec, basis, data, preferred_element_type=F32).astype(BF16)


def on_device_plain(
    source, forward_x, forward_y_basis, forward_z, inverse_x, inverse_y_basis, inverse_z,
    values_x, values_y, values_z,
):
    iy, ig, iz = lax.axis_index("gx"), lax.axis_index("gy"), lax.axis_index("gz")
    move = functools.partial(lax.all_to_all, tiled=True)
    step = move(source, "gx", split_axis=0, concat_axis=1)
    step = move(plain(step, forward_y_basis, "qy,zyx->zqx"), "gx", split_axis=1, concat_axis=0)
    step = move(step, "gy", split_axis=1, concat_axis=2)
    step = plain(step, forward_x, "px,zqx->zqp")
    step = plain(move(step, "gz", split_axis=2, concat_axis=0), forward_z, "rz,zqp->rqp")
    _, rows, cols = step.shape
    first = (iy * lax.axis_size("gy") + ig) * rows
    lam_y = lax.dynamic_slice_in_dim(values_y, first, rows)
    lam_x = lax.dynamic_slice_in_dim(values_x, iz * cols, cols)
    denom = values_z[:, None, None] + lam_y[None, :, None] + lam_x[None, None, :]
    step = (step.astype(F32) / denom).astype(BF16)
    step = move(plain(step, inverse_z, "zr,rqp->zqp"), "gz", split_axis=0, concat_axis=2)
    step = plain(step, inverse_x, "xp,zqp->zqx")
    step = move(step, "gy", split_axis=2, concat_axis=1)
    step = move(step, "gx", split_axis=0, concat_axis=1)
    return move(plain(step, inverse_y_basis, "yq,zqx->zyx"), "gx", split_axis=1, concat_axis=0)


def solution(mesh):
    def run(source, *rest):
        ny, ng, nz = (mesh.shape[a] for a in ("gx", "gy", "gz"))
        depth, size_y, size_x = source.shape
        fits = (
            size_x // nz % 128 == 0
            and size_x // ng % 128 == 0
            and depth // nz % (ROWS * sum(FORWARD_SIZES)) == 0
            and depth // nz % (ROWS * sum(BACKWARD_SIZES)) == 0
            and size_y // ny // ng % 16 == 0
            and all(n & (n - 1) == 0 for n in (ny, ng, nz))
        )
        body = on_device_plain
        if fits:

            def body(*args):
                return on_device(*args)

        step = jax.shard_map(
            body,
            mesh=mesh,
            in_specs=(P("gz", "gx", "gy"),) + (P(),) * 9,
            out_specs=P("gz", "gx", "gy"),
            check_vma=False,
        )
        return step(source, *rest)

    return run
```

```python
import functools

import jax
import jax.numpy as jnp
from jax import lax
from jax.experimental import pallas as pl
from jax.experimental.pallas import tpu as pltpu
from jax.sharding import PartitionSpec as P


FORWARD_SIZES = (1,)*8
BACKWARD_SIZES = (1,)*8
AHEAD = {'S':2,'W':2}
SENDS = {"S": "gx", "G": "gy", "Z": "gz", "W": "gz", "H": "gy", "T": "gx"}
ROWS = 8
F32 = jnp.float32
BF16 = jnp.bfloat16


def dot(a, b):
    return jnp.dot(a, b, preferred_element_type=F32)


def params(**kw):
    return pltpu.CompilerParams(vmem_limit_bytes=48 * 1024 * 1024, **kw)


def cost(flops, nbytes):
    return pl.CostEstimate(flops=flops, bytes_accessed=nbytes, transcendentals=0)


ANY = pl.BlockSpec(memory_space=pl.ANY)


def chunks(depth, sizes):
    rows = [n * depth // sum(sizes) for n in sizes]
    by_z = [0, len(rows) - 1] + list(range(1, len(rows) - 1))
    starts = [0] * len(rows)
    for a, b in zip(by_z, by_z[1:]):
        starts[b] = starts[a] + rows[a]
    return rows, starts, by_z


def forward_order():
    n = len(FORWARD_SIZES)
    ahead = AHEAD["S"]
    steps = [f"{kind}{c}" for c in range(ahead) for kind in "CS"]
    for c in range(n):
        steps += [f"F{c}", f"G{c}"]
        steps += [f"{kind}{c + ahead}" for kind in "CS" if c + ahead < n]
        steps += [f"A{c}", f"Z{c}"]
    return steps


def backward_order():
    n = len(BACKWARD_SIZES)
    steps = [f"W{c}" for c in range(AHEAD["W"])]
    for c in range(n):
        steps += [f"B{c}", f"H{c}"] + [f"W{c + AHEAD['W']}"] * (c + AHEAD["W"] < n)
        steps += [f"R{c - 3}"] * (c > 2) + [f"P{c}", f"T{c}"]
    return steps + [f"R{c}" for c in range(n - 3, n)]


def partners(count):
    return list(range(2, count)) + [1]


def places(index, count):
    return [index ^ k for k in range(count)]


def cut(ref, height, row, width, col):
    return ref[
        pl.ds(pl.multiple_of(row * height, height), height),
        pl.ds(pl.multiple_of(col * width, width), width),
    ]


def forward_y_kernel(*refs, count, outs):
    place, pieces, basis, out = refs[0], refs[1 : 1 + count], refs[1 + count], refs[-outs:]
    steps, rows, cols = pieces[0].shape
    width = basis.shape[0] // count // outs
    own = jnp.concatenate(
        [
            jnp.concatenate([cut(basis, width, r, rows, c) for c in places(place[0], count)], axis=1)
            for r in places(place[0] * outs + place[1], outs)
        ],
        axis=0,
    )

    def pair(i, carry):
        z = 2 * i
        rhs = jnp.concatenate(
            [jnp.concatenate([ref[z], ref[z + 1]], axis=1) for ref in pieces], axis=0
        )
        acc = dot(own, rhs).astype(BF16)
        for k in range(outs):
            block = acc[k * width : (k + 1) * width]
            out[k][z] = block[:, :cols]
            out[k][z + 1] = block[:, cols:]
        return carry

    lax.fori_loop(0, steps // 2, pair, 0, unroll=4)


def forward_y(place, own, start, others, basis, outs, after=()):
    zc, rows, cols = others[0].shape
    count = 1 + len(others)
    q = basis.shape[0] // count
    first = start // ROWS
    spec = pl.BlockSpec((ROWS, rows, cols), lambda i, s: (i, 0, 0))
    return pl.pallas_call(
        functools.partial(forward_y_kernel, count=count, outs=outs),
        grid_spec=pltpu.PrefetchScalarGridSpec(
            num_scalar_prefetch=1,
            grid=(zc // ROWS,),
            in_specs=[pl.BlockSpec((ROWS, rows, cols), lambda i, s: (i + first, 0, 0))]
            + [spec] * len(others)
            + [pl.BlockSpec(basis.shape, lambda i, s: (0, 0))]
            + [ANY] * len(after),
            out_specs=[pl.BlockSpec((ROWS, q // outs, cols), lambda i, s: (i, 0, 0))] * outs,
        ),
        out_shape=[jax.ShapeDtypeStruct((zc, q // outs, cols), BF16)] * outs,
        compiler_params=params(),
        cost_estimate=cost(2 * zc * q * basis.shape[1] * cols, 2 * zc * cols * (basis.shape[1] + q)),
        name="forward_y",
    )(place, own, *others, basis, *after)


def along_x_kernel(*refs, count, outs, axes):
    place, pieces, basis = refs[0], refs[1 : 1 + count], refs[1 + count]
    out, scratch = refs[-1 - outs : -1], refs[-1]
    a, b, cols = pieces[0].shape
    pitch = scratch.shape[1] // a
    width = basis.shape[0] // outs
    lhs = jnp.concatenate([ref[...].reshape(a * b, cols) for ref in pieces], axis=1)
    for k, row in enumerate(places(place[axes[1]], outs)):
        rhs = jnp.concatenate(
            [cut(basis, width, row, cols, c) for c in places(place[axes[0]], count)], axis=1
        )
        acc = lax.dot_general(lhs, rhs, (((1,), (1,)), ((), ())), preferred_element_type=F32)
        for i in range(a):
            scratch[k % 2, i * pitch : i * pitch + b, :] = acc[i * b : (i + 1) * b]
        for j in range(b):
            out[k][j] = scratch[k % 2, pl.ds(j, a, stride=pitch), :].astype(BF16)


def along_x(place, pieces, basis, outs, rows_first, after=()):
    cols = pieces[0].shape[2]
    width = basis.shape[0] // outs
    zc, q = pieces[0].shape[:2] if rows_first else pieces[0].shape[1::-1]
    z_major = ((ROWS, q), lambda i, s: (i, 0, 0))
    q_major = ((q, ROWS), lambda i, s: (0, i, 0))
    src, dst = (z_major, q_major) if rows_first else (q_major, z_major)
    shape = (q, zc, width) if rows_first else (zc, q, width)
    pitch = src[0][1] + 8
    return pl.pallas_call(
        functools.partial(
            along_x_kernel, count=len(pieces), outs=outs, axes=(1, 2) if rows_first else (2, 1)
        ),
        grid_spec=pltpu.PrefetchScalarGridSpec(
            num_scalar_prefetch=1,
            grid=(zc // ROWS,),
            in_specs=[pl.BlockSpec(src[0] + (cols,), src[1])] * len(pieces)
            + [pl.BlockSpec(basis.shape, lambda i, s: (0, 0))]
            + [ANY] * len(after),
            out_specs=[pl.BlockSpec(dst[0] + (width,), dst[1])] * outs,
            scratch_shapes=[pltpu.VMEM((2, src[0][0] * pitch, width), F32)],
        ),
        out_shape=[jax.ShapeDtypeStruct(shape, BF16)] * outs,
        compiler_params=params(),
        cost_estimate=cost(2 * zc * q * basis.shape[0] * basis.shape[1], 2 * zc * q * sum(basis.shape)),
        name="along_x",
    )(place, *pieces, basis, *after)


def lines_kernel(*refs, count, outs, step):
    place, lam_y, pieces = refs[0], refs[1], refs[2 : 2 + count]
    forward, inverse, base = refs[2 + count : 5 + count]
    out, there, back_again = refs[-2 - outs : -2], refs[-2], refs[-1]
    first = pl.program_id(0) * step
    depth, cols = base.shape

    @pl.when(pl.program_id(0) == 0)
    def _():
        n = there.shape[0]
        size = depth // n
        for k, block in enumerate(places(place[2], n)):
            there[k] = forward[:, pl.ds(pl.multiple_of(block * size, size), size)]
            back_again[k * size : (k + 1) * size] = inverse[pl.ds(pl.multiple_of(block * size, size), size), :]

    lhs = jnp.concatenate([there[k] for k in range(there.shape[0])], axis=1)
    for q in range(0, step, 2):
        rhs = jnp.concatenate(
            [jnp.concatenate([ref[q], ref[q + 1]], axis=1) for ref in pieces], axis=0
        )
        acc = dot(lhs, rhs).astype(BF16).astype(F32)
        left = acc[:, :cols] / (base[...] + lam_y[first + q])
        right = acc[:, cols:] / (base[...] + lam_y[first + q + 1])
        back = dot(back_again[...], jnp.concatenate([left, right], axis=1).astype(BF16)).astype(BF16)
        row = 0
        for ref in out:
            stop = row + ref.shape[1]
            ref[q] = back[row:stop, :cols]
            ref[q + 1] = back[row:stop, cols:]
            row = stop


def lines(place, pieces, forward, inverse, base, lam_y, parts, sizes):
    q, _, cols = pieces[0].shape
    depth = forward.shape[0]
    step = 16
    spec = lambda n: pl.BlockSpec((step, n, cols), lambda i, s, t: (i, 0, 0))
    whole = lambda x: pl.BlockSpec(x.shape, lambda i, s, t: (0, 0))
    outs = [n for _ in range(parts) for n in sizes]
    return pl.pallas_call(
        functools.partial(lines_kernel, count=len(pieces), outs=len(outs), step=step),
        grid_spec=pltpu.PrefetchScalarGridSpec(
            num_scalar_prefetch=2,
            grid=(q // step,),
            in_specs=[spec(p.shape[1]) for p in pieces] + [whole(forward), whole(inverse), whole(base)],
            out_specs=[spec(n) for n in outs],
            scratch_shapes=[
                pltpu.VMEM((parts, depth, depth // parts), BF16),
                pltpu.VMEM((depth, depth), BF16),
            ],
        ),
        out_shape=[jax.ShapeDtypeStruct((q, n, cols), BF16) for n in outs],
        compiler_params=params(),
        cost_estimate=cost(4 * q * cols * depth * depth, 4 * q * cols * depth),
        name="lines",
    )(place, lam_y, *pieces, forward, inverse, base)


def inverse_y_kernel(*refs, count, adds, to):
    place, pieces, basis = refs[0], refs[1 : 1 + count], refs[1 + count]
    partials, out, there = refs[2 + count : 2 + count + adds], refs[-2], refs[-1]
    _, q, cols = pieces[0].shape
    rows = out.shape[1]
    own = cut(basis, rows, place[0] ^ to, count * q, place[0])
    for ref, k in zip(pieces, places(place[1], count)):
        there[k] = ref[...]

    def pair(i, carry):
        z = 2 * i
        rhs = jnp.concatenate(
            [jnp.concatenate([there[k, z], there[k, z + 1]], axis=1) for k in range(count)], axis=0
        )
        acc = dot(own, rhs)
        left, right = acc[:, :cols], acc[:, cols:]
        for ref in partials:
            left = left + ref[z].astype(F32)
            right = right + ref[z + 1].astype(F32)
        out[z] = left.astype(BF16)
        out[z + 1] = right.astype(BF16)
        return carry

    lax.fori_loop(0, out.shape[0] // 2, pair, 0, unroll=4)


def inverse_y(place, pieces, basis, to, rows, after=(), partials=(), into=None, start=0, depth=None):
    zc, q, cols = pieces[0].shape
    first = start // ROWS
    part = pl.BlockSpec((ROWS, rows, cols), lambda i, s: (i, 0, 0))
    extra = [] if into is None else [into]
    count = len(pieces)
    return pl.pallas_call(
        functools.partial(inverse_y_kernel, count=count, adds=len(partials), to=to),
        grid_spec=pltpu.PrefetchScalarGridSpec(
            num_scalar_prefetch=1,
            grid=(zc // ROWS,),
            in_specs=[pl.BlockSpec((ROWS, q, cols), lambda i, s: (i, 0, 0))] * count
            + [pl.BlockSpec(basis.shape, lambda i, s: (0, 0))]
            + [part] * len(partials)
            + [ANY] * (len(extra) + len(after)),
            out_specs=pl.BlockSpec((ROWS, rows, cols), lambda i, s: (i + first, 0, 0)),
            scratch_shapes=[pltpu.VMEM((count, ROWS, q, cols), BF16)],
        ),
        out_shape=jax.ShapeDtypeStruct((depth or zc, rows, cols), BF16),
        input_output_aliases={count + 2 + len(partials): 0} if extra else {},
        compiler_params=params(),
        cost_estimate=cost(2 * zc * rows * count * q * cols, 2 * zc * cols * (count * q + rows)),
        name="inverse_y",
    )(place, *pieces, basis, *partials, *extra, *after)


def swap(value, axis, k):
    count = lax.axis_size(axis)
    return lax.ppermute(value, axis, [(i, i ^ k) for i in range(count)])


def exchange(step, pieces):
    axis = SENDS[step[0]]
    out = list(pieces)
    for k in partners(len(pieces)):
        out[k] = swap(pieces[k], axis, k)
    return out


def copy_kernel(source, out):
    out[...] = source[...]


def copy_rows(source, start, count):
    first = start // ROWS
    block = (ROWS,) + source.shape[1:]
    return pl.pallas_call(
        copy_kernel,
        grid=(count // block[0],),
        in_specs=[pl.BlockSpec(block, lambda i: (i + first, 0, 0))],
        out_specs=pl.BlockSpec(block, lambda i: (i, 0, 0)),
        out_shape=jax.ShapeDtypeStruct((count,) + source.shape[1:], BF16),
        compiler_params=params(),
        name="copy_rows",
    )(source)


def on_device(
    source, forward_x, forward_y_basis, forward_z, inverse_x, inverse_y_basis, inverse_z,
    values_x, values_y, values_z,
):
    ny, ng, nz = lax.axis_size("gx"), lax.axis_size("gy"), lax.axis_size("gz")
    iy, ig, iz = lax.axis_index("gx"), lax.axis_index("gy"), lax.axis_index("gz")
    place = jnp.stack([iy, ig, iz]).astype(jnp.int32)
    depth, rows, _ = source.shape
    slim = values_y.shape[0] // ny // ng
    width = values_x.shape[0] // nz
    lam_y = lax.dynamic_slice_in_dim(values_y, (iy * ng + ig) * slim, slim)
    lam_x = lax.dynamic_slice_in_dim(values_x, iz * width, width)
    base = values_z[:, None] + lam_x[None, :]

    sizes, starts, by_z = chunks(depth, FORWARD_SIZES)
    have = {}
    for step in forward_order():
        kind, c = step[0], int(step[1:])
        if kind in "CFA":
            if kind == "C":
                have[step] = copy_rows(source, starts[c], sizes[c])
            elif kind == "F":
                have[step] = forward_y(
                    place, source, starts[c], have[f"S{c}"], forward_y_basis, ng
                )
            else:
                have[step] = along_x(place, have[f"G{c}"], forward_x, nz, True)
        elif kind == "S":
            have[step] = exchange(step, [have[f"C{c}"]] * ny)[1:]
        else:
            have[step] = exchange(step, have[f"{'F' if kind == 'G' else 'A'}{c}"])

    flat = [have[f"Z{c}"][k] for k in range(nz) for c in by_z]
    sizes, starts, by_z = chunks(depth, BACKWARD_SIZES)
    count = len(sizes)
    flat = lines(place, flat, forward_z, inverse_z, base, lam_y, nz, [sizes[c] for c in by_z])

    result = None
    for step in backward_order():
        kind, c = step[0], int(step[1:])
        if kind == "W":
            have[step] = exchange(step, [flat[k * count + by_z.index(c)] for k in range(nz)])
        elif kind == "H":
            have[step] = exchange(step, have[f"B{c}"])
        elif kind == "T":
            have[step] = exchange(step, [None] + have[f"P{c}"])[1:]
        elif kind == "P":
            have[step] = [None] * (ny - 1)
            for k in partners(ny):
                have[step][k - 1] = inverse_y(place, have[f"H{c}"], inverse_y_basis, k, rows)
        else:
            if kind == "B":
                have[step] = along_x(place, have[f"W{c}"], inverse_x, ng, False)
            else:
                result = inverse_y(
                    place, have[f"H{c}"], inverse_y_basis, 0, rows, (),
                    have[f"T{c}"], result, starts[c], depth,
                )
    return result


def plain(data, basis, spec):
    return jnp.einsum(spec, basis, data, preferred_element_type=F32).astype(BF16)


def on_device_plain(
    source, forward_x, forward_y_basis, forward_z, inverse_x, inverse_y_basis, inverse_z,
    values_x, values_y, values_z,
):
    iy, ig, iz = lax.axis_index("gx"), lax.axis_index("gy"), lax.axis_index("gz")
    move = functools.partial(lax.all_to_all, tiled=True)
    step = move(source, "gx", split_axis=0, concat_axis=1)
    step = move(plain(step, forward_y_basis, "qy,zyx->zqx"), "gx", split_axis=1, concat_axis=0)
    step = move(step, "gy", split_axis=1, concat_axis=2)
    step = plain(step, forward_x, "px,zqx->zqp")
    step = plain(move(step, "gz", split_axis=2, concat_axis=0), forward_z, "rz,zqp->rqp")
    _, rows, cols = step.shape
    first = (iy * lax.axis_size("gy") + ig) * rows
    lam_y = lax.dynamic_slice_in_dim(values_y, first, rows)
    lam_x = lax.dynamic_slice_in_dim(values_x, iz * cols, cols)
    denom = values_z[:, None, None] + lam_y[None, :, None] + lam_x[None, None, :]
    step = (step.astype(F32) / denom).astype(BF16)
    step = move(plain(step, inverse_z, "zr,rqp->zqp"), "gz", split_axis=0, concat_axis=2)
    step = plain(step, inverse_x, "xp,zqp->zqx")
    step = move(step, "gy", split_axis=2, concat_axis=1)
    step = move(step, "gx", split_axis=0, concat_axis=1)
    return move(plain(step, inverse_y_basis, "yq,zqx->zyx"), "gx", split_axis=1, concat_axis=0)


def solution(mesh):
    def run(source, *rest):
        ny, ng, nz = (mesh.shape[a] for a in ("gx", "gy", "gz"))
        depth, size_y, size_x = source.shape
        fits = (
            size_x // nz % 128 == 0
            and size_x // ng % 128 == 0
            and depth // nz % (ROWS * sum(FORWARD_SIZES)) == 0
            and depth // nz % (ROWS * sum(BACKWARD_SIZES)) == 0
            and size_y // ny // ng % 16 == 0
            and all(n & (n - 1) == 0 for n in (ny, ng, nz))
        )
        body = on_device_plain
        if fits:

            def body(*args):
                return on_device(*args)

        step = jax.shard_map(
            body,
            mesh=mesh,
            in_specs=(P("gz", "gx", "gy"),) + (P(),) * 9,
            out_specs=P("gz", "gx", "gy"),
            check_vma=False,
        )
        return step(source, *rest)

    return run
```
